32 devices in a mesh: tok: 16 (over z, x, core), blk: 2 (over y).
Axes of the slice: x: 2, y: 2, z: 4, core: 2. Of those that a mesh axis runs over, the one named last changes fastest.
Arguments:
- activations: bfloat16 [2048, 7168], P('tok', 'blk'), may hold values from -600 to 600
- signs: float32 [7168], P('blk'), may hold values from -1 to 1, as said below
Outputs:
- hessian: float32 [7168, 7168], P('tok', 'blk')
- incoherence: float32 [7168], P('blk')
- largest_ratio: float32 [], replicated
The draws below stay inside these ranges and needn't reach their ends.
Inputs may be any that keep to these rules, and one draw needn't show every extreme that they name: `signs`: every entry is -1 or 1.
All inputs are finite; a program needn't handle non-finite values.
Results may differ from the reference program's by a relative error of at most 0.0037.
Values may be sent and summed in bfloat16 or wider, within the bound.
No kernel may reach another device: no remote copies, remote signals or barrier semaphores. Data moves between devices by JAX's collectives and lax.ppermute only.
A program may use at most 640 MiB of HBM per device.

```python
import math
import jax
import jax.numpy as jnp
from jax import lax

WALSH = 512
MIX = 14
FEATURES = 7168
TOKENS = 2048


def draw_activations(key, part):
    noise_key, scale_key = jax.random.split(key, 2)
    position = jnp.arange(TOKENS, dtype=jnp.float32) / TOKENS
    ramp = jnp.exp(math.log(3.0) * position)[:, None]
    row_scale = jnp.exp(jax.random.uniform(scale_key, (TOKENS, 1), jnp.float32, 0.0, math.log(10.0)))
    values = jnp.clip(jax.random.normal(noise_key, (TOKENS, FEATURES), jnp.float32), -5.0, 5.0)
    return (values * ramp * row_scale).astype(jnp.bfloat16)


def draw_signs(key, part):
    coins = jax.random.randint(key, (FEATURES,), 0, 2)
    return (2 * coins - 1).astype(jnp.float32)


def setup_inputs(seed: int = 0) -> dict:
    seeds = jax.random.split(jax.random.key(seed), 3)
    return {
        "activations": draw_activations(jax.random.fold_in(seeds[2], 71), 0),
        "signs": draw_signs(jax.random.fold_in(seeds[2], 71), 0),
    }


EPS = 1e-06
DAMP = 0.01

def walsh_table(length):
    position = jnp.arange(length, dtype=jnp.int32)
    parity = jnp.zeros((length, length), jnp.int32)
    for bit_number in range(length.bit_length() - 1):
        parity = parity + (position[:, None] >> bit_number & 1) * (position[None, :] >> bit_number & 1)
    return (1 - 2 * (parity % 2)).astype(jnp.float32)

def cosine_table(length):
    rows_idx = jnp.arange(length, dtype=jnp.float32)[:, None]
    columns = jnp.arange(length, dtype=jnp.float32)[None, :]
    table = math.sqrt(2.0 / length) * jnp.cos(math.pi * (columns + 0.5) * rows_idx / length)
    return jnp.where(rows_idx == 0.0, table * math.sqrt(0.5), table)

def reference(activations, signs):
    signed = activations * signs.astype(jnp.bfloat16)[None, :]
    tokens_total = activations.shape[0]
    values = signed.astype(jnp.float32).reshape(tokens_total, WALSH, MIX)
    values = jnp.einsum('tba,ka->tbk', values, cosine_table(MIX), precision=lax.Precision.HIGHEST)
    values = jnp.einsum('tbk,cb->tck', values, walsh_table(WALSH) / math.sqrt(WALSH), precision=lax.Precision.HIGHEST)
    rotated = values.reshape(tokens_total, FEATURES).astype(jnp.bfloat16)
    gram_matrix = lax.dot_general(rotated, rotated, (((0,), (0,)), ((), ())), preferred_element_type=jnp.float32)
    on_diag = jnp.eye(FEATURES, dtype=jnp.bool_)
    trace_total = jnp.sum(jnp.diagonal(gram_matrix))
    diag_mean = trace_total / FEATURES + EPS
    hessian = gram_matrix / diag_mean + DAMP * on_diag.astype(jnp.float32)
    column_peak = lax.optimization_barrier(jnp.max(jnp.where(on_diag, 0.0, jnp.abs(gram_matrix)), axis=0))
    incoherence = column_peak / diag_mean
    return (hessian, incoherence, jnp.max(incoherence))
```

```python
import math

import jax
import jax.numpy as jnp
import numpy as np
from jax import lax
from jax.sharding import PartitionSpec as P

WALSH = 512
MIX = 14
EPS = 1e-06
DAMP = 0.01
LANES = 128


def walsh_np(order):
    index = np.arange(order)
    parity = np.zeros((order, order), np.int64)
    for bit in range(order.bit_length() - 1):
        parity += (index[:, None] >> bit & 1) * (index[None, :] >> bit & 1)
    return (1 - 2 * (parity % 2)).astype(np.float64)


def cosine_np(order):
    k = np.arange(order, dtype=np.float64)[:, None]
    n = np.arange(order, dtype=np.float64)[None, :]
    table = math.sqrt(2.0 / order) * np.cos(math.pi * (n + 0.5) * k / order)
    table[0] *= math.sqrt(0.5)
    return table


def walsh_jnp(order):
    index = jnp.arange(order, dtype=jnp.int32)
    joint = index[:, None] & index[None, :]
    for bit in (16, 8, 4, 2, 1):
        joint = joint ^ (joint >> bit)
    return (1 - 2 * (joint & 1)).astype(jnp.float32)


def inner_tables(inner):
    cos = (cosine_np(MIX).T / math.sqrt(WALSH)).astype(np.float32)
    high = np.asarray(cos.astype(jnp.bfloat16))
    low = np.asarray((cos - high.astype(np.float32)).astype(jnp.bfloat16))
    walsh = walsh_jnp(inner).astype(jnp.bfloat16)
    tables = []
    for part in (high, low):
        rows = jnp.repeat(jnp.repeat(walsh, MIX, axis=0), MIX, axis=1)
        tables.append(rows * jnp.tile(jnp.asarray(part), (inner, inner)))
    return tables


def pair_route(count, step):
    return [(i, i ^ step) for i in range(count)]


def per_device(activations, signs):
    tokens, width = activations.shape
    blocks = lax.axis_size("blk")
    blk = lax.axis_index("blk")
    groups = lax.axis_size("tok")
    tok = lax.axis_index("tok")
    features = width * blocks
    inner = math.gcd(width // MIX, WALSH // blocks, 64)
    inner_width = inner * MIX
    outer = width // inner_width

    signed = activations * signs.astype(jnp.bfloat16)[None, :]
    tables = inner_tables(inner)

    def spread(part):
        stacked = jnp.concatenate(
            [part[:, i * inner_width : (i + 1) * inner_width] for i in range(outer)], axis=0
        )
        mixed = sum(jnp.dot(stacked, t, preferred_element_type=jnp.float32) for t in tables)
        parts = [mixed[i * tokens : (i + 1) * tokens] for i in range(outer)]
        step = 1
        while step < outer:
            parts = [
                parts[i ^ step] - parts[i] if i & step else parts[i] + parts[i ^ step]
                for i in range(outer)
            ]
            step *= 2
        return jnp.concatenate(parts, axis=1)

    total = None
    for step in range(blocks):
        block = signed if step == 0 else lax.ppermute(signed, "blk", pair_route(blocks, step))
        joint = blk & (blk ^ step)
        parity = sum(joint >> bit & 1 for bit in range(max(1, blocks.bit_length() - 1))) & 1
        sign = jnp.where(parity == 1, -1.0, 1.0).astype(jnp.float32)
        term = spread(block) * sign
        total = term if total is None else total + term
    rotated = total.astype(jnp.bfloat16)

    wide = rotated.astype(jnp.float32)
    trace_total = jnp.sum(wide * wide, axis=0, keepdims=True).reshape(-1, LANES)
    trace_total = jnp.sum(trace_total, axis=0)
    for axis, count in (("blk", blocks), ("tok", groups)):
        step = 1
        while step < count:
            trace_total += lax.ppermute(trace_total, axis, pair_route(count, step))
            step *= 2
    trace_total = jnp.sum(trace_total)
    diag_mean = trace_total / features + EPS

    all_tokens = lax.all_gather(rotated, "tok", axis=0, tiled=True)
    row_count = features // groups
    owner = tok * row_count // width
    offset = tok * row_count - owner * width
    own_slice = lax.dynamic_slice_in_dim(all_tokens, offset, row_count, 1)
    row_slice = jnp.where(blk == owner, own_slice, 0).astype(jnp.bfloat16)
    for step in range(1, blocks):
        route = []
        for t in range(groups):
            source = t * row_count // width
            route.append((t * blocks + source, t * blocks + (source ^ step)))
        row_slice = row_slice + lax.ppermute(own_slice, ("tok", "blk"), route)

    gram = lax.dot_general(
        row_slice, all_tokens, (((0,), (0,)), ((), ())), preferred_element_type=jnp.float32
    )
    rows = tok * row_count + jnp.arange(row_count, dtype=jnp.int32)[:, None]
    columns = blk * width + jnp.arange(width, dtype=jnp.int32)[None, :]
    on_diag = rows == columns
    row_peak = jnp.max(jnp.where(on_diag, 0.0, jnp.abs(gram)), axis=1)
    hessian = gram / diag_mean + DAMP * on_diag.astype(jnp.float32)
    step = 1
    while step < blocks:
        row_peak = jnp.maximum(row_peak, lax.ppermute(row_peak, "blk", pair_route(blocks, step)))
        step *= 2
    peaks = row_peak[None, :]
    step = 1
    while step < groups:
        other = lax.ppermute(peaks, "tok", pair_route(groups, step))
        upper = (tok & step) != 0
        peaks = jnp.concatenate(
            [jnp.where(upper, other, peaks), jnp.where(upper, peaks, other)], axis=0
        )
        step *= 2
    peaks = peaks.reshape(features)
    incoherence = lax.dynamic_slice_in_dim(peaks, blk * width, width, 0) / diag_mean
    return hessian, incoherence, jnp.max(peaks) / diag_mean


def solution(mesh):
    in_specs = (P("tok", "blk"), P("blk"))
    out_specs = (P("tok", "blk"), P("blk"), P())
    return jax.shard_map(
        per_device, mesh=mesh, in_specs=in_specs, out_specs=out_specs, check_vma=False
    )
```

```python
import math

import jax
import jax.numpy as jnp
import numpy as np
from jax import lax
from jax.sharding import PartitionSpec as P

WALSH = 512
MIX = 14
EPS = 1e-06
DAMP = 0.01
LANES = 128


def walsh_np(order):
    index = np.arange(order)
    parity = np.zeros((order, order), np.int64)
    for bit in range(order.bit_length() - 1):
        parity += (index[:, None] >> bit & 1) * (index[None, :] >> bit & 1)
    return (1 - 2 * (parity % 2)).astype(np.float64)


def cosine_np(order):
    k = np.arange(order, dtype=np.float64)[:, None]
    n = np.arange(order, dtype=np.float64)[None, :]
    table = math.sqrt(2.0 / order) * np.cos(math.pi * (n + 0.5) * k / order)
    table[0] *= math.sqrt(0.5)
    return table


def inner_tables(inner):
    cos = (cosine_np(MIX).T / math.sqrt(WALSH)).astype(np.float32)
    high = np.asarray(cos.astype(jnp.bfloat16))
    low = np.asarray((cos - high.astype(np.float32)).astype(jnp.bfloat16))
    walsh = walsh_np(inner).astype(jnp.bfloat16)
    spot = np.arange(inner * MIX)
    pick_walsh = (spot[:, None] // MIX == np.arange(inner)[None, :]).astype(jnp.bfloat16)
    pick_cos = (spot[:, None] % MIX == np.arange(MIX)[None, :]).astype(jnp.bfloat16)
    wide_walsh = np.repeat(walsh, MIX, axis=1)
    wide_cos = np.concatenate([np.tile(high, (1, inner)), np.tile(low, (1, inner))], axis=1)
    pick_walsh, pick_cos, wide_walsh, wide_cos = lax.optimization_barrier(
        tuple(jnp.asarray(v) for v in (pick_walsh, pick_cos, wide_walsh, wide_cos))
    )
    signs = jnp.dot(pick_walsh, wide_walsh, preferred_element_type=jnp.float32)
    values = jnp.dot(pick_cos, wide_cos, preferred_element_type=jnp.float32)
    width = inner * MIX
    return lax.optimization_barrier(
        tuple((signs * values[:, i * width : (i + 1) * width]).astype(jnp.bfloat16) for i in range(2))
    )


def pair_route(count, step):
    return [(i, i ^ step) for i in range(count)]


def ring_routes(groups):
    pairs = groups // 2
    order = list(range(0, pairs, 2)) + list(range(1, pairs, 2))[::-1]
    onward = []
    for i, pair in enumerate(order):
        after = order[(i + 1) % pairs]
        onward += [(2 * pair + c, 2 * after + c) for c in range(2)]
    return onward, [(b, a) for a, b in onward]


def per_device(activations, signs):
    tokens, width = activations.shape
    blocks = lax.axis_size("blk")
    blk = lax.axis_index("blk")
    groups = lax.axis_size("tok")
    tok = lax.axis_index("tok")
    features = width * blocks
    inner = math.gcd(width // MIX, WALSH // blocks, 64)
    inner_width = inner * MIX
    outer = width // inner_width

    signed = activations * signs.astype(jnp.bfloat16)[None, :]
    tables = inner_tables(inner)

    def spread(part):
        count = part.shape[0]
        stacked = jnp.concatenate(
            [part[:, i * inner_width : (i + 1) * inner_width] for i in range(outer)], axis=0
        )
        mixed = sum(jnp.dot(stacked, t, preferred_element_type=jnp.float32) for t in tables)
        parts = [mixed[i * count : (i + 1) * count] for i in range(outer)]
        step = 1
        while step < outer:
            parts = [
                parts[i ^ step] - parts[i] if i & step else parts[i] + parts[i ^ step]
                for i in range(outer)
            ]
            step *= 2
        return jnp.concatenate(parts, axis=1)

    def swap(part):
        return [lax.ppermute(part, "blk", pair_route(blocks, step)) for step in range(1, blocks)]

    def walsh_sign(joint):
        parity = sum(joint >> bit & 1 for bit in range(max(1, blocks.bit_length() - 1))) & 1
        return jnp.where(parity == 1, -1.0, 1.0).astype(jnp.float32)

    def rotate(part, others):
        total = spread(part) * walsh_sign(blk)
        for step in range(1, blocks):
            total = total + spread(others[step - 1]) * walsh_sign(blk & (blk ^ step))
        return total.astype(jnp.bfloat16)

    half = tokens // 2
    early, late = signed[:half], signed[half:]
    early_others = swap(early)
    late, _ = lax.optimization_barrier((late, early_others))
    first, second = rotate(early, early_others), rotate(late, swap(late))

    trace_total = 0.0
    for part in (first, second):
        wide = part.astype(jnp.float32)
        trace_total += jnp.sum(jnp.sum(wide * wide, axis=0).reshape(-1, LANES), axis=0)

    row_count = features // groups
    owner = tok * row_count // width
    offset = tok * row_count - owner * width
    sibling = pair_route(groups, 1)
    onward, back = ring_routes(groups)
    hops = groups // 4

    def with_rows(pieces):
        pieces = pieces + [lax.ppermute(p, "tok", sibling) for p in pieces]
        block = jnp.concatenate(pieces, axis=0)
        own_rows = lax.dynamic_slice_in_dim(block, offset, row_count, 1)
        row_slice = jnp.where(blk == owner, own_rows, 0).astype(jnp.bfloat16)
        for step in range(1, blocks):
            route = []
            for t in range(groups):
                source = t * row_count // width
                route.append((t * blocks + source, t * blocks + (source ^ step)))
            row_slice = row_slice + lax.ppermute(own_rows, ("tok", "blk"), route)
        return pieces, row_slice

    def partial_gram(*chunks):
        return lax.dot_general(
            jnp.concatenate([rows for _, rows in chunks], axis=0),
            jnp.concatenate([p for pieces, _ in chunks for p in pieces], axis=0),
            (((0,), (0,)), ((), ())),
            preferred_element_type=jnp.float32,
        )

    gram = lax.optimization_barrier(partial_gram(with_rows([first, second])))
    held = []
    ahead, behind = [first, second], [first, second]
    for hop in range(1, hops + 1):
        if hop < hops:
            moved_on, moved_back = [], []
            for i in range(2):
                moved_on.append(lax.ppermute(ahead[i], "tok", onward))
                moved_back.append(lax.ppermute(behind[i], "tok", back))
            ahead, behind = moved_on, moved_back
            if hop < hops - 1:
                arrived = partial_gram(with_rows(ahead + behind))
            else:
                arrived = partial_gram(with_rows([ahead[0], behind[0]]))
                held = [with_rows([ahead[1], behind[1]])]
            gram = lax.optimization_barrier(gram + arrived)
        else:
            last = [lax.ppermute(ahead[0], "tok", onward), lax.ppermute(behind[1], "tok", back)]
            gram = gram + partial_gram(*held, with_rows(last))

    rows = tok * row_count + jnp.arange(row_count, dtype=jnp.int32)[:, None]
    columns = blk * width + jnp.arange(width, dtype=jnp.int32)[None, :]
    on_diag = rows == columns
    row_peak = jnp.max(jnp.where(on_diag, 0.0, jnp.abs(gram)), axis=1)
    for bit in range(blocks.bit_length() - 1):
        message = jnp.concatenate([row_peak, trace_total])
        other = lax.ppermute(message, "blk", pair_route(blocks, 1 << bit))
        row_peak = jnp.maximum(row_peak, other[:row_count])
        trace_total = trace_total + other[row_count:]
    peaks = row_peak[None, :]
    for bit in range(groups.bit_length() - 1):
        step = 1 << bit
        message = jnp.concatenate([peaks.reshape(-1), trace_total])
        other = lax.ppermute(message, "tok", pair_route(groups, step))
        trace_total = trace_total + other[step * row_count :]
        other = other[: step * row_count].reshape(step, row_count)
        upper = (tok & step) != 0
        peaks = jnp.concatenate(
            [jnp.where(upper, other, peaks), jnp.where(upper, peaks, other)], axis=0
        )
    peaks = peaks.reshape(features)
    diag_mean = jnp.sum(trace_total) / features + EPS
    hessian = gram / diag_mean + DAMP * on_diag.astype(jnp.float32)
    incoherence = lax.dynamic_slice_in_dim(peaks, blk * width, width, 0) / diag_mean
    return hessian, incoherence, jnp.max(peaks) / diag_mean


def solution(mesh):
    in_specs = (P("tok", "blk"), P("blk"))
    out_specs = (P("tok", "blk"), P("blk"), P())
    return jax.shard_map(
        per_device, mesh=mesh, in_specs=in_specs, out_specs=out_specs, check_vma=False
    )
```
